32 devices in a mesh: grp: 1, blk: 8 (over z, y), node: 4 (over x, core), pair: 1.
Axes of the slice: x: 2, y: 2, z: 4, core: 2. Of those that a mesh axis runs over, the one named last changes fastest.
Arguments:
- query: bfloat16 [4608, 1280], P(('grp', 'blk', 'node'), 'pair'), may hold values from -600 to 600
- key: bfloat16 [4608, 1280], P(('grp', 'blk', 'node'), 'pair'), may hold values from -25 to 25
- value: bfloat16 [4608, 1280], P(('grp', 'blk', 'node'), 'pair'), may hold values from -6 to 6
- out_weight: bfloat16 [1280, 1280], P('pair'), may hold values from -0.15625 to 0.15625
Outputs:
- mixed: bfloat16 [4608, 1280], P(('grp', 'blk', 'node', 'pair'))
The draws below stay inside these ranges and needn't reach their ends.
All inputs are finite; a program needn't handle non-finite values.
Results may differ from the reference program's by a relative error of at most 0.011.
Values may be sent and summed in bfloat16 or wider, within the bound.
A program may use at most 128 MiB of HBM per device.

```python
import math
import jax
import jax.numpy as jnp
from jax import lax

D = 1280
HEADS = 20
HD = 64
TOKENS = 4608


def key_rows(key):
    base = jnp.clip(jax.random.normal(jax.random.fold_in(key, 101), (TOKENS, D), jnp.float32), -4.5, 4.5)
    return base.astype(jnp.bfloat16)


def draw_key(key, part):
    return key_rows(key)


def draw_query(key, part):
    drawn = jax.random.normal(jax.random.fold_in(key, 105), (TOKENS, D), jnp.float32) * 2.5
    return jnp.clip(drawn, -12.0, 12.0).astype(jnp.bfloat16)


def block_levels(own_key, extent, shards, least, top_value):
    gain = 1.0
    for dim, shards_of in shards:
        steps = jax.random.uniform(jax.random.fold_in(jax.random.fold_in(own_key, 6), dim), (shards_of,), jnp.float32, least / len(shards), top_value / len(shards))
        gain = gain * jnp.repeat(jnp.exp(steps), extent[dim] // shards_of).reshape((-1,) + (1,) * (len(extent) - 1 - dim))
    return gain


def scatter_about(rng, shape, scale, reach, cuts=(), held_as=jnp.bfloat16):
    array = scale * jax.random.normal(rng, shape, jnp.float32)
    if cuts:
        array = array * block_levels(rng, shape, cuts, -0.22, 0.18)
    return jnp.clip(array, -reach, reach).astype(held_as)


def setup_inputs(seed: int = 0, part: int = 0) -> dict:
    keys = jax.random.split(jax.random.key(seed), 5)
    own_keys = jax.random.split(jax.random.fold_in(keys[4], part), 5)
    return {
        "query": draw_query(jax.random.fold_in(jax.random.fold_in(keys[4], part), 71), part),
        "key": draw_key(jax.random.fold_in(jax.random.fold_in(keys[4], part), 71), part),
        "value": scatter_about(own_keys[2], (TOKENS, D), 1.0, 6.0, ((0, 32),)),
        "out_weight": scatter_about(keys[3], (D, D), D ** -0.5, 0.15625),
    }


def reference(query, key, value, out_weight):
    scale = 1.0 / math.sqrt(HD)
    q_heads = query.reshape(TOKENS, HEADS, HD).transpose(1, 0, 2)
    k_heads = key.reshape(TOKENS, HEADS, HD).transpose(1, 0, 2)
    v_heads = value.reshape(TOKENS, HEADS, HD).transpose(1, 0, 2)

    def one_head(operands):
        q_one, k_one, v_one = operands
        scores = jnp.dot(q_one, k_one.T, preferred_element_type=jnp.float32) * scale
        peak = lax.optimization_barrier(jnp.max(scores, axis=1, keepdims=True))
        expo = jnp.exp(scores - peak)
        total = lax.optimization_barrier(jnp.sum(expo, axis=1, keepdims=True))
        return jnp.dot(expo.astype(jnp.bfloat16), v_one, preferred_element_type=jnp.float32) / total
    heads_out = lax.map(one_head, (q_heads, k_heads, v_heads))
    attn = heads_out.transpose(1, 0, 2).reshape(TOKENS, D).astype(jnp.bfloat16)
    return jnp.dot(attn, out_weight, preferred_element_type=jnp.float32).astype(jnp.bfloat16)
```

```python
import functools
import math

import jax
import jax.numpy as jnp
from jax import lax
from jax.experimental import pallas as pl
from jax.experimental.pallas import tpu as pltpu
from jax.sharding import PartitionSpec as P

HD = 64
WIDE = 2 * HD


def groups_of(blk, heads):
    return max(g for g in range(1, blk + 1) if blk % g == 0 and heads % g == 0)


def kernel(
    G, B, N,
    q_ref, kv_ref, o_ref,
    qz, kvz, qbuf, kvbuf, vbuf, opack,
    z_send, z_recv, q_send, q_recv, kv_send, kv_recv, o_send, o_recv,
):
    H, R2, _ = q_ref.shape
    R = kv_ref.shape[1]
    hg = H // G
    PL = B // G
    inner = PL // N
    NS = kvbuf.shape[0]
    blk, node = lax.axis_index("blk"), lax.axis_index("node")
    z = blk // inner
    p = (blk % inner) * N + node

    def peer(zz, pp):
        return {"blk": zz * inner + pp // N, "node": pp % N}

    def remote(src, dst, send, recv, zz, pp):
        return pltpu.make_async_remote_copy(
            src_ref=src, dst_ref=dst, send_sem=send, recv_sem=recv,
            device_id=peer(zz, pp), device_id_type=pl.DeviceIdType.MESH,
        )

    def phase1(dz):
        g = lax.rem(z + dz, G)
        heads = pl.ds(g * hg, hg)
        return (
            remote(kv_ref.at[heads], kvz.at[dz - 1], z_send.at[dz - 1, 0], z_recv.at[dz - 1, 0], g, p),
            remote(q_ref.at[heads], qz.at[dz - 1], z_send.at[dz - 1, 1], z_recv.at[dz - 1, 1], g, p),
        )

    for dz in range(1, G):
        for c in phase1(dz):
            c.start()

    def first(pp):
        return (pp * H) // B

    def last(pp):
        return (pp * H + H - 1) // B

    def phase2(s, act):
        src_z = lax.rem(z - s + G, G)
        b = src_z * PL + p

        def kv_src(h):
            return kv_ref.at[z * hg + h] if s == 0 else kvz.at[s - 1, h]

        def one(dp, _):
            pp = lax.rem(p + dp, PL)
            f, l = first(pp), last(pp)
            for slot in range(NS):
                @pl.when(f + slot <= l)
                def _():
                    act(remote(kv_src(f + slot), kvbuf.at[slot, b], kv_send.at[s, dp, slot], kv_recv.at[slot, b], z, pp))
            return 0

        lax.fori_loop(1, PL, one, 0)
        for h in range(hg):
            n = h * B + b
            pp = n // H
            u = n - pp * H
            src = q_ref.at[z * hg + h] if s == 0 else qz.at[s - 1, h]

            @pl.when(pp != p)
            def _():
                act(remote(src, qbuf.at[u], q_send.at[s, h], q_recv.at[u], z, pp))

    def own(s):
        b = lax.rem(z - s + G, G) * PL + p
        for slot in range(NS):
            @pl.when(first(p) + slot <= last(p))
            def _():
                h = first(p) + slot
                src = kv_ref.at[z * hg + h] if s == 0 else kvz.at[s - 1, h]
                pltpu.make_async_copy(src, kvbuf.at[slot, b], kv_recv.at[slot, b]).start()
        for h in range(hg):
            n = h * B + b
            u = n - p * H
            src = q_ref.at[z * hg + h] if s == 0 else qz.at[s - 1, h]

            @pl.when(n // H == p)
            def _():
                pltpu.make_async_copy(src, qbuf.at[u], q_recv.at[u]).start()

    for s in range(G):
        if s > 0:
            for c in phase1(s):
                c.wait_recv()
        phase2(s, lambda c: c.start())
        own(s)

    def wait_q(u, _):
        pltpu.make_async_copy(qbuf.at[u], qbuf.at[u], q_recv.at[u]).wait()
        return 0

    lax.fori_loop(0, H, wait_q, 0)
    lanes = lax.broadcasted_iota(jnp.int32, (R, WIDE), 1)
    for slot in range(NS):
        @pl.when(first(p) + slot <= last(p))
        def _():
            def wait_kv(b, _):
                pltpu.make_async_copy(kvbuf.at[slot, b], kvbuf.at[slot, b], kv_recv.at[slot, b]).wait()
                vbuf[slot, b] = jnp.where(lanes < HD, jnp.ones((), vbuf.dtype), kvbuf[slot, b])
                return 0
            lax.fori_loop(0, B, wait_kv, 0)

    half = lax.broadcasted_iota(jnp.int32, (R2, WIDE), 1) < HD
    scale = 1.0 / math.sqrt(HD)

    def unit(u):
        n = p * H + u
        h = n // B
        slot = h - first(p)
        both = qbuf[u].astype(jnp.float32) * scale
        zero = jnp.zeros_like(both)
        queries = jnp.concatenate(
            [jnp.where(half, both, zero), jnp.where(half, pltpu.roll(both, HD, 1), zero)], axis=0
        ).astype(jnp.bfloat16)
        scores = lax.dot_general(
            queries, kvbuf[slot].reshape(B * R, WIDE), (((1,), (1,)), ((), ())),
            preferred_element_type=jnp.float32,
        )
        peak = jnp.max(scores, axis=1, keepdims=True)
        expo = jnp.exp(scores - peak).astype(jnp.bfloat16)
        weighted = jnp.dot(expo, vbuf[slot].reshape(B * R, WIDE), preferred_element_type=jnp.float32)
        turned = pltpu.roll(weighted, HD, 1)
        opack[u] = jnp.where(
            half, turned[:R2] / weighted[:R2], weighted[R2:] / turned[R2:]
        ).astype(opack.dtype)

    def give(u, act):
        n = p * H + u
        h = n // B
        b = n - h * B
        zz, pp = b // PL, lax.rem(b, PL)
        mine = jnp.logical_and(zz == z, pp == p)
        row = z * hg + h

        @pl.when(jnp.logical_not(mine))
        def _():
            act(remote(opack.at[u], o_ref.at[row], o_send.at[u], o_recv.at[row], zz, pp))

        return mine, row

    def turn(u, _):
        unit(u)
        mine, row = give(u, lambda c: c.start())

        @pl.when(mine)
        def _():
            pltpu.make_async_copy(opack.at[u], o_ref.at[row], o_recv.at[row]).start()

        return 0

    lax.fori_loop(0, H, turn, 0)

    for dz in range(1, G):
        for c in phase1(dz):
            c.wait_send()
    for s in range(G):
        phase2(s, lambda c: c.wait_send())

    def end(u, _):
        give(u, lambda c: c.wait_send())
        pltpu.make_async_copy(o_ref.at[u], o_ref.at[u], o_recv.at[u]).wait()
        return 0

    lax.fori_loop(0, H, end, 0)


def per_device(query, key, value, out_weight):
    R, features = query.shape
    H = features // HD
    R2 = R // 2
    nblk, N = lax.axis_size("blk"), lax.axis_size("node")
    B = nblk * N
    G = groups_of(nblk, H)
    hg = H // G
    NS = (H + B - 2) // B + 1
    q = query.reshape(2, R2, H, HD).transpose(2, 1, 0, 3).reshape(H, R2, WIDE)
    kv = jnp.concatenate(
        [key.reshape(R, H, HD), value.reshape(R, H, HD)], axis=2
    ).transpose(1, 0, 2)
    dma = pltpu.SemaphoreType.DMA
    bf = jnp.bfloat16
    out = pl.pallas_call(
        functools.partial(kernel, G, B, N),
        out_shape=jax.ShapeDtypeStruct((H, R2, WIDE), bf),
        in_specs=[pl.BlockSpec(memory_space=pltpu.VMEM)] * 2,
        out_specs=pl.BlockSpec(memory_space=pltpu.VMEM),
        scratch_shapes=[
            pltpu.VMEM((max(G - 1, 1), hg, R2, WIDE), bf),
            pltpu.VMEM((max(G - 1, 1), hg, R, WIDE), bf),
            pltpu.VMEM((H, R2, WIDE), bf),
            pltpu.VMEM((NS, B, R, WIDE), bf),
            pltpu.VMEM((NS, B, R, WIDE), bf),
            pltpu.VMEM((H, R2, WIDE), bf),
            dma((max(G - 1, 1), 2)),
            dma((max(G - 1, 1), 2)),
            dma((G, hg)),
            dma((H,)),
            dma((G, B // G, NS)),
            dma((NS, B)),
            dma((H,)),
            dma((H,)),
        ],
        compiler_params=pltpu.CompilerParams(
            has_side_effects=True, vmem_limit_bytes=60 * 1024 * 1024
        ),
        name="attention",
    )(q, kv)
    attn = out.reshape(H, R2, 2, HD).transpose(2, 1, 0, 3).reshape(R, features)
    return lax.psum_scatter(
        jnp.dot(attn, out_weight, preferred_element_type=jnp.float32).astype(jnp.bfloat16),
        "pair",
        scatter_dimension=0,
        tiled=True,
    )


def solution(mesh):
    in_specs = (
        P(("grp", "blk", "node"), "pair"),
        P(("grp", "blk", "node"), "pair"),
        P(("grp", "blk", "node"), "pair"),
        P("pair", None),
    )
    out_specs = P(("grp", "blk", "node", "pair"), None)
    return jax.shard_map(
        per_device, mesh=mesh, in_specs=in_specs, out_specs=out_specs, check_vma=False
    )
```

```python
import functools
import math

import jax
import jax.numpy as jnp
from jax import lax
from jax.experimental import pallas as pl
from jax.experimental.pallas import tpu as pltpu
from jax.sharding import PartitionSpec as P

HD = 64
WIDE = 2 * HD


def groups_of(blk, heads):
    return max(g for g in range(1, blk + 1) if blk % g == 0 and heads % g == 0)


def kernel(
    G, B, N,
    query_ref, key_ref, value_ref, weight_ref, mixed_ref,
    qp, kvp, qz, kvz, qbuf, kvbuf, vbuf, qfull, peaks, accum, opack, oin, attn, weight,
    z_send, z_recv, q_send, q_recv, kv_send, kv_recv, o_send, o_recv, w_sem,
):
    H, R2, _ = qp.shape
    R = kvp.shape[1]
    hg = H // G
    PL = B // G
    inner = PL // N
    NS = kvbuf.shape[0]
    C = math.gcd(H, B)
    blk, node = lax.axis_index("blk"), lax.axis_index("node")
    z = blk // inner
    p = (blk % inner) * N + node
    bf, f32 = jnp.bfloat16, jnp.float32

    load_weight = pltpu.make_async_copy(weight_ref, weight, w_sem)
    load_weight.start()

    def peer(zz, pp):
        return {"blk": zz * inner + pp // N, "node": pp % N}

    def remote(src, dst, send, recv, zz, pp):
        return pltpu.make_async_remote_copy(
            src_ref=src, dst_ref=dst, send_sem=send, recv_sem=recv,
            device_id=peer(zz, pp), device_id_type=pl.DeviceIdType.MESH,
        )

    half = lax.broadcasted_iota(jnp.int32, (R2, WIDE), 1) < HD
    wide_half = lax.broadcasted_iota(jnp.int32, (R, WIDE), 1) < HD

    for pair in range(H // 2):
        columns = slice(pair * WIDE, (pair + 1) * WIDE)
        block = query_ref[:, columns].astype(f32)
        turned = pltpu.roll(block, HD, 1)
        qp[2 * pair] = jnp.where(half, block[:R2], turned[R2:]).astype(bf)
        qp[2 * pair + 1] = jnp.where(half, turned[:R2], block[R2:]).astype(bf)
    for pair in range(H // 2):
        columns = slice(pair * WIDE, (pair + 1) * WIDE)
        keys = key_ref[:, columns].astype(f32)
        values = value_ref[:, columns].astype(f32)
        kvp[2 * pair] = jnp.where(wide_half, keys, pltpu.roll(values, HD, 1)).astype(bf)
        kvp[2 * pair + 1] = jnp.where(wide_half, pltpu.roll(keys, HD, 1), values).astype(bf)

    def phase1(dz, part):
        g = lax.rem(z + dz, G)
        src, dst = ((qp, qz), (kvp, kvz))[part]
        return remote(
            src.at[pl.ds(g * hg, hg)], dst.at[dz - 1], z_send.at[dz - 1, part], z_recv.at[dz - 1, part], g, p
        )

    for part in range(2):
        for dz in range(1, G):
            phase1(dz, part).start()

    def first(pp):
        return (pp * H) // B

    def last(pp):
        return (pp * H + H - 1) // B

    def plane(s):
        return lax.rem(z - s + G, G)

    def q_src(s, h):
        return qp.at[z * hg + h] if s == 0 else qz.at[s - 1, h]

    def kv_src(s, h):
        return kvp.at[z * hg + h] if s == 0 else kvz.at[s - 1, h]

    def share_q(s, act):
        b = plane(s) * PL + p
        for h in range(hg):
            n = h * B + b
            pp = n // H
            u = n - pp * H

            @pl.when(pp != p)
            def _():
                act(remote(q_src(s, h), qbuf.at[u], q_send.at[s, h], q_recv.at[u], z, pp))

    def own_q(s):
        b = plane(s) * PL + p
        for h in range(hg):
            n = h * B + b

            @pl.when(n // H == p)
            def _():
                pltpu.make_async_copy(q_src(s, h), qbuf.at[n - p * H], q_recv.at[n - p * H]).start()

    def share_kv(s, act):
        b = plane(s) * PL + p

        def one(dp, _):
            pp = lax.rem(p + dp, PL)
            for slot in range(NS):
                @pl.when(first(pp) + slot <= last(pp))
                def _():
                    act(remote(
                        kv_src(s, first(pp) + slot), kvbuf.at[slot, b],
                        kv_send.at[s, dp, slot], kv_recv.at[slot, b], z, pp,
                    ))
            return 0

        lax.fori_loop(1, PL, one, 0)

    def own_kv(s):
        b = plane(s) * PL + p
        for slot in range(NS):
            @pl.when(first(p) + slot <= last(p))
            def _():
                pltpu.make_async_copy(kv_src(s, first(p) + slot), kvbuf.at[slot, b], kv_recv.at[slot, b]).start()

    start = lambda c: c.start()
    share_q(0, start)
    own_q(0)
    share_kv(0, start)
    own_kv(0)
    for s in range(1, G):
        phase1(s, 0).wait_recv()
        share_q(s, start)
        own_q(s)

    scale = 1.0 / math.sqrt(HD)

    def take_q(u, _):
        pltpu.make_async_copy(qbuf.at[u], qbuf.at[u], q_recv.at[u]).wait()
        both = qbuf[u].astype(f32) * scale
        zero = jnp.zeros_like(both)
        qfull[u] = jnp.concatenate(
            [jnp.where(half, both, zero), jnp.where(half, pltpu.roll(both, HD, 1), zero)], axis=0
        ).astype(bf)
        return 0

    def take_kv(s):
        for slot in range(NS):
            @pl.when(first(p) + slot <= last(p))
            def _():
                def one(i, _):
                    b = plane(s) * PL + i
                    pltpu.make_async_copy(kvbuf.at[slot, b], kvbuf.at[slot, b], kv_recv.at[slot, b]).wait()
                    vbuf[slot, i] = jnp.where(wide_half, jnp.ones((), bf), kvbuf[slot, b])
                    return 0
                lax.fori_loop(0, PL, one, 0)

    def give(u, act):
        n = p * H + u
        h = n // B
        b = n - h * B
        zz, pp = b // PL, lax.rem(b, PL)
        mine = jnp.logical_and(zz == z, pp == p)
        row = z * hg + h

        @pl.when(jnp.logical_not(mine))
        def _():
            act(remote(opack.at[u], oin.at[row], o_send.at[u], o_recv.at[row], zz, pp))

        return mine, row

    def attend(s, t):
        slot = (p * H + t * C) // B - first(p)
        units = pl.ds(t * C, C)
        queries = qfull[units].reshape(C * R, WIDE)
        keys = kvbuf[slot, pl.ds(plane(s) * PL, PL)].reshape(PL * R, WIDE)
        scores = lax.dot_general(
            queries, keys, (((1,), (1,)), ((), ())), preferred_element_type=f32
        )
        peak = jnp.max(scores, axis=1, keepdims=True)
        if s > 0:
            before = peaks[units].reshape(C * R, WIDE)
            peak = jnp.maximum(before[:, :1], peak)
        expo = jnp.exp(scores - peak).astype(bf)
        total = jnp.dot(expo, vbuf[slot].reshape(PL * R, WIDE), preferred_element_type=f32)
        if s > 0:
            total = total + accum[units].reshape(C * R, WIDE) * jnp.exp(before - peak)
        if s < G - 1:
            peaks[units] = jnp.broadcast_to(peak, (C * R, WIDE)).reshape(C, R, WIDE)
            accum[units] = total.reshape(C, R, WIDE)
            return
        turned = pltpu.roll(total, HD, 1)
        for i in range(C):
            low, high = slice(i * R, i * R + R2), slice(i * R + R2, (i + 1) * R)
            opack[t * C + i] = jnp.where(
                half, turned[low] / total[low], total[high] / turned[high]
            ).astype(bf)
        for i in range(C):
            u = t * C + i
            mine, row = give(u, start)

            @pl.when(mine)
            def _():
                pltpu.make_async_copy(opack.at[u], oin.at[row], o_recv.at[row]).start()

    for s in range(G):
        if s + 1 < G:
            phase1(s + 1, 1).wait_recv()
            share_kv(s + 1, start)
            own_kv(s + 1)
        if s == 0:
            lax.fori_loop(0, H, take_q, 0)
        take_kv(s)

        def turn(t, _):
            attend(s, t)
            return 0

        lax.fori_loop(0, H // C, turn, 0)

    for dz in range(1, G):
        for part in range(2):
            phase1(dz, part).wait_send()
    for s in range(G):
        share_q(s, lambda c: c.wait_send())
        share_kv(s, lambda c: c.wait_send())

    def end(u, _):
        give(u, lambda c: c.wait_send())
        pltpu.make_async_copy(oin.at[u], oin.at[u], o_recv.at[u]).wait()
        return 0

    load_weight.wait()
    lax.fori_loop(0, H, end, 0)
    for pair in range(H // 2):
        even, odd = oin[2 * pair].astype(f32), oin[2 * pair + 1].astype(f32)
        attn[:, pair * WIDE:(pair + 1) * WIDE] = jnp.concatenate(
            [
                jnp.where(half, even, pltpu.roll(odd, HD, 1)),
                jnp.where(half, pltpu.roll(even, HD, 1), odd),
            ],
            axis=0,
        ).astype(bf)
    mixed_ref[...] = jnp.dot(attn[...], weight[...], preferred_element_type=f32).astype(bf)


def per_device(query, key, value, out_weight):
    R, features = query.shape
    H = features // HD
    R2 = R // 2
    nblk, N = lax.axis_size("blk"), lax.axis_size("node")
    B = nblk * N
    G = groups_of(nblk, H)
    hg = H // G
    NS = (H + B - 2) // B + 1
    dma = pltpu.SemaphoreType.DMA
    bf, f32 = jnp.bfloat16, jnp.float32
    vmem = pl.BlockSpec(memory_space=pltpu.VMEM)
    mixed = pl.pallas_call(
        functools.partial(kernel, G, B, N),
        out_shape=jax.ShapeDtypeStruct((R, out_weight.shape[1]), bf),
        in_specs=[vmem, vmem, vmem, pl.BlockSpec(memory_space=pl.ANY)],
        out_specs=vmem,
        scratch_shapes=[
            pltpu.VMEM((H, R2, WIDE), bf),
            pltpu.VMEM((H, R, WIDE), bf),
            pltpu.VMEM((max(G - 1, 1), hg, R2, WIDE), bf),
            pltpu.VMEM((max(G - 1, 1), hg, R, WIDE), bf),
            pltpu.VMEM((H, R2, WIDE), bf),
            pltpu.VMEM((NS, B, R, WIDE), bf),
            pltpu.VMEM((NS, B // G, R, WIDE), bf),
            pltpu.VMEM((H, R, WIDE), bf),
            pltpu.VMEM((H, R, WIDE), f32),
            pltpu.VMEM((H, R, WIDE), f32),
            pltpu.VMEM((H, R2, WIDE), bf),
            pltpu.VMEM((H, R2, WIDE), bf),
            pltpu.VMEM((R, features), bf),
            pltpu.VMEM(out_weight.shape, bf),
            dma((max(G - 1, 1), 2)),
            dma((max(G - 1, 1), 2)),
            dma((G, hg)),
            dma((H,)),
            dma((G, B // G, NS)),
            dma((NS, B)),
            dma((H,)),
            dma((H,)),
            dma(()),
        ],
        compiler_params=pltpu.CompilerParams(
            has_side_effects=True, vmem_limit_bytes=60 * 1024 * 1024
        ),
        name="attention",
    )(query, key, value, out_weight)
    return lax.psum_scatter(mixed, "pair", scatter_dimension=0, tiled=True)


def solution(mesh):
    in_specs = (
        P(("grp", "blk", "node"), "pair"),
        P(("grp", "blk", "node"), "pair"),
        P(("grp", "blk", "node"), "pair"),
        P("pair", None),
    )
    out_specs = P(("grp", "blk", "node", "pair"), None)
    return jax.shard_map(
        per_device, mesh=mesh, in_specs=in_specs, out_specs=out_specs, check_vma=False
    )
```

```python
import functools
import math

import jax
import jax.numpy as jnp
from jax import lax
from jax.experimental import pallas as pl
from jax.experimental.pallas import tpu as pltpu
from jax.sharding import PartitionSpec as P

HD = 64
WIDE = 2 * HD


def groups_of(blk, heads):
    return max(g for g in range(1, blk + 1) if blk % g == 0 and heads % g == 0)


def kernel(
    G, B, N,
    query_ref, key_ref, value_ref, weight_ref, mixed_ref,
    qp, kvp, kvz, qbuf, kvbuf, vbuf, qfull, peaks, accum, opack, oin, attn, weight,
    z_send, z_recv, q_send, q_recv, kv_send, kv_recv, o_send, o_recv, w_sem,
):
    H, R2, _ = qp.shape
    R = kvp.shape[1]
    hg = H // G
    PL = B // G
    inner = PL // N
    NS = kvbuf.shape[0]
    C = math.gcd(H, B)
    blk, node = lax.axis_index("blk"), lax.axis_index("node")
    z = blk // inner
    p = (blk % inner) * N + node
    bf, f32 = jnp.bfloat16, jnp.float32

    load_weight = pltpu.make_async_copy(weight_ref, weight, w_sem)
    load_weight.start()
    barrier = pltpu.get_barrier_semaphore()
    here = blk * N + node

    def greet(d, _):
        other = lax.rem(here + d, B)
        pl.semaphore_signal(
            barrier, inc=1, device_id={"blk": other // N, "node": lax.rem(other, N)},
            device_id_type=pl.DeviceIdType.MESH,
        )
        return 0

    lax.fori_loop(1, B, greet, 0)

    def peer(zz, pp):
        return {"blk": zz * inner + pp // N, "node": pp % N}

    def remote(src, dst, send, recv, zz, pp):
        return pltpu.make_async_remote_copy(
            src_ref=src, dst_ref=dst, send_sem=send, recv_sem=recv,
            device_id=peer(zz, pp), device_id_type=pl.DeviceIdType.MESH,
        )

    half = lax.broadcasted_iota(jnp.int32, (R2, WIDE), 1) < HD
    wide_half = lax.broadcasted_iota(jnp.int32, (R, WIDE), 1) < HD

    for pair in range(H // 2):
        columns = slice(pair * WIDE, (pair + 1) * WIDE)
        block = query_ref[:, columns].astype(f32)
        turned = pltpu.roll(block, HD, 1)
        qp[2 * pair] = jnp.where(half, block[:R2], turned[R2:]).astype(bf)
        qp[2 * pair + 1] = jnp.where(half, turned[:R2], block[R2:]).astype(bf)
    for pair in range(H // 2):
        columns = slice(pair * WIDE, (pair + 1) * WIDE)
        keys = key_ref[:, columns].astype(f32)
        values = value_ref[:, columns].astype(f32)
        kvp[2 * pair] = jnp.where(wide_half, keys, pltpu.roll(values, HD, 1)).astype(bf)
        kvp[2 * pair + 1] = jnp.where(wide_half, pltpu.roll(keys, HD, 1), values).astype(bf)

    pl.semaphore_wait(barrier, B - 1)

    def send_q(i, act):
        row = lax.rem((z + 1) * hg + i, H)
        zz = row // hg
        n = (row - zz * hg) * B + here
        pp = n // H
        u = n - pp * H
        mine = jnp.logical_and(zz == z, pp == p)

        @pl.when(jnp.logical_not(mine))
        def _():
            act(remote(qp.at[row], qbuf.at[u], q_send.at[row], q_recv.at[u], zz, pp))

        return mine, row, u

    def start_q(i, _):
        mine, row, u = send_q(i, lambda c: c.start())

        @pl.when(mine)
        def _():
            pltpu.make_async_copy(qp.at[row], qbuf.at[u], q_recv.at[u]).start()

        return 0

    lax.fori_loop(0, H, start_q, 0)

    def phase1(dz):
        g = lax.rem(z + dz, G)
        return remote(
            kvp.at[pl.ds(g * hg, hg)], kvz.at[dz - 1], z_send.at[dz - 1], z_recv.at[dz - 1], g, p
        )

    for dz in range(1, G):
        phase1(dz).start()

    def first(pp):
        return (pp * H) // B

    def last(pp):
        return (pp * H + H - 1) // B

    def kv_src(s, h):
        return kvp.at[z * hg + h] if s == 0 else kvz.at[s - 1, h]

    def share_kv(s, act):
        b = s * PL + p

        def one(dp, _):
            pp = lax.rem(p + dp, PL)
            for slot in range(NS):
                @pl.when(first(pp) + slot <= last(pp))
                def _():
                    act(remote(
                        kv_src(s, first(pp) + slot), kvbuf.at[slot, b],
                        kv_send.at[s, dp, slot], kv_recv.at[slot, b], z, pp,
                    ))
            return 0

        lax.fori_loop(1, PL, one, 0)

    def own_kv(s):
        b = s * PL + p
        for slot in range(NS):
            @pl.when(first(p) + slot <= last(p))
            def _():
                pltpu.make_async_copy(kv_src(s, first(p) + slot), kvbuf.at[slot, b], kv_recv.at[slot, b]).start()

    start = lambda c: c.start()
    share_kv(0, start)
    own_kv(0)

    scale = 1.0 / math.sqrt(HD)

    def take_q(u, _):
        pltpu.make_async_copy(qbuf.at[u], qbuf.at[u], q_recv.at[u]).wait()
        both = qbuf[u].astype(f32) * scale
        zero = jnp.zeros_like(both)
        qfull[u] = jnp.concatenate(
            [jnp.where(half, both, zero), jnp.where(half, pltpu.roll(both, HD, 1), zero)], axis=0
        ).astype(bf)
        return 0

    def take_kv(low, high):
        for slot in range(NS):
            @pl.when(first(p) + slot <= last(p))
            def _():
                def one(b, _):
                    pltpu.make_async_copy(kvbuf.at[slot, b], kvbuf.at[slot, b], kv_recv.at[slot, b]).wait()
                    vbuf[slot, b] = jnp.where(wide_half, jnp.ones((), bf), kvbuf[slot, b])
                    return 0
                lax.fori_loop(low * PL, high * PL, one, 0)

    def give(u, act):
        n = p * H + u
        h = n // B
        b = n - h * B
        zz, pp = b // PL, lax.rem(b, PL)
        mine = jnp.logical_and(zz == z, pp == p)
        row = z * hg + h

        @pl.when(jnp.logical_not(mine))
        def _():
            act(remote(opack.at[u], oin.at[row], o_send.at[u], o_recv.at[row], zz, pp))

        return mine, row

    def attend(low, high, t):
        slot = (p * H + t * C) // B - first(p)
        keys = kvbuf[slot, low * PL:high * PL].reshape((high - low) * PL * R, WIDE)
        values = vbuf[slot, low * PL:high * PL].reshape((high - low) * PL * R, WIDE)

        def product(c):
            return lax.dot_general(
                qfull[t * C + c], keys, (((1,), (1,)), ((), ())), preferred_element_type=f32
            )

        def soften(c, scores):
            u = t * C + c
            peak = jnp.max(scores, axis=1, keepdims=True)
            if low > 0:
                before = peaks[u]
                peak = jnp.maximum(before[:, :1], peak)
            expo = jnp.exp(scores - peak).astype(bf)
            total = jnp.dot(expo, values, preferred_element_type=f32)
            if low > 0:
                total = total + accum[u] * jnp.exp(before - peak)
            if high < G:
                peaks[u] = jnp.broadcast_to(peak, (R, WIDE))
                accum[u] = total
                return
            turned = pltpu.roll(total, HD, 1)
            opack[u] = jnp.where(
                half, turned[:R2] / total[:R2], total[R2:] / turned[R2:]
            ).astype(bf)

        scores = product(0)
        for c in range(C):
            ahead = product(c + 1) if c + 1 < C else None
            soften(c, scores)
            scores = ahead
        if high < G:
            return
        for i in range(C):
            u = t * C + i
            mine, row = give(u, start)

            @pl.when(mine)
            def _():
                pltpu.make_async_copy(opack.at[u], oin.at[row], o_recv.at[row]).start()

    def relay(s):
        if s < G:
            phase1(s).wait_recv()
            share_kv(s, start)
            own_kv(s)

    stages = [(s, s + 1) for s in range(min(G, 2))]
    stages += [(s, min(s + 2, G)) for s in range(2, G, 2)]
    turns = H // C
    relay(1)
    lax.fori_loop(0, H, take_q, 0)
    for low, high in stages:
        take_kv(low, high)

        def turn(t, _):
            attend(low, high, t)
            return 0

        if high == 2 and low == 1 and G > 3:
            lax.fori_loop(0, turns // 2, turn, 0)
            relay(3)
            lax.fori_loop(turns // 2, turns, turn, 0)
        else:
            lax.fori_loop(0, turns, turn, 0)
        if high == 1:
            relay(2)
        if high >= 2:
            for s in range(high + 2, min(high + 4, G)):
                relay(s)

    for dz in range(1, G):
        phase1(dz).wait_send()
    for s in range(G):
        share_kv(s, lambda c: c.wait_send())

    def end_q(i, _):
        send_q(i, lambda c: c.wait_send())
        return 0

    lax.fori_loop(0, H, end_q, 0)

    def end(u, _):
        give(u, lambda c: c.wait_send())
        pltpu.make_async_copy(oin.at[u], oin.at[u], o_recv.at[u]).wait()
        return 0

    load_weight.wait()
    lax.fori_loop(0, H, end, 0)
    for pair in range(H // 2):
        even, odd = oin[2 * pair].astype(f32), oin[2 * pair + 1].astype(f32)
        attn[:, pair * WIDE:(pair + 1) * WIDE] = jnp.concatenate(
            [
                jnp.where(half, even, pltpu.roll(odd, HD, 1)),
                jnp.where(half, pltpu.roll(even, HD, 1), odd),
            ],
            axis=0,
        ).astype(bf)
    mixed_ref[...] = jnp.dot(attn[...], weight[...], preferred_element_type=f32).astype(bf)


def per_device(query, key, value, out_weight):
    R, features = query.shape
    H = features // HD
    R2 = R // 2
    nblk, N = lax.axis_size("blk"), lax.axis_size("node")
    B = nblk * N
    G = groups_of(nblk, H)
    hg = H // G
    NS = (H + B - 2) // B + 1
    dma = pltpu.SemaphoreType.DMA
    bf, f32 = jnp.bfloat16, jnp.float32
    vmem = pl.BlockSpec(memory_space=pltpu.VMEM)
    mixed = pl.pallas_call(
        functools.partial(kernel, G, B, N),
        out_shape=jax.ShapeDtypeStruct((R, out_weight.shape[1]), bf),
        in_specs=[vmem, vmem, vmem, pl.BlockSpec(memory_space=pl.ANY)],
        out_specs=vmem,
        scratch_shapes=[
            pltpu.VMEM((H, R2, WIDE), bf),
            pltpu.VMEM((H, R, WIDE), bf),
            pltpu.VMEM((max(G - 1, 1), hg, R, WIDE), bf),
            pltpu.VMEM((H, R2, WIDE), bf),
            pltpu.VMEM((NS, B, R, WIDE), bf),
            pltpu.VMEM((NS, B, R, WIDE), bf),
            pltpu.VMEM((H, R, WIDE), bf),
            pltpu.VMEM((H, R, WIDE), f32),
            pltpu.VMEM((H, R, WIDE), f32),
            pltpu.VMEM((H, R2, WIDE), bf),
            pltpu.VMEM((H, R2, WIDE), bf),
            pltpu.VMEM((R, features), bf),
            pltpu.VMEM(out_weight.shape, bf),
            dma((max(G - 1, 1),)),
            dma((max(G - 1, 1),)),
            dma((H,)),
            dma((H,)),
            dma((G, B // G, NS)),
            dma((NS, B)),
            dma((H,)),
            dma((H,)),
            dma(()),
        ],
        compiler_params=pltpu.CompilerParams(
            collective_id=0, has_side_effects=True, vmem_limit_bytes=60 * 1024 * 1024
        ),
        name="attention",
    )(query, key, value, out_weight)
    return lax.psum_scatter(mixed, "pair", scatter_dimension=0, tiled=True)


def solution(mesh):
    in_specs = (
        P(("grp", "blk", "node"), "pair"),
        P(("grp", "blk", "node"), "pair"),
        P(("grp", "blk", "node"), "pair"),
        P("pair", None),
    )
    out_specs = P(("grp", "blk", "node", "pair"), None)
    return jax.shard_map(
        per_device, mesh=mesh, in_specs=in_specs, out_specs=out_specs, check_vma=False
    )
```

```python
import functools
import math

import jax
import jax.numpy as jnp
from jax import lax
from jax.experimental import pallas as pl
from jax.experimental.pallas import tpu as pltpu
from jax.sharding import PartitionSpec as P

HD = 64
WIDE = 2 * HD


def groups_of(blk, heads):
    return max(g for g in range(1, blk + 1) if blk % g == 0 and heads % g == 0)


def kernel(
    G, B, N,
    query_ref, key_ref, value_ref, weight_ref, mixed_ref,
    qp, kvp, kvz, qbuf, kvbuf, vbuf, qfull, peaks, accum, opack, oin, attn, weight,
    z_send, z_recv, q_send, q_recv, kv_send, kv_recv, o_send, o_recv, w_sem,
):
    H, R2, _ = qp.shape
    R = kvp.shape[1]
    hg = H // G
    PL = B // G
    inner = PL // N
    NS = kvbuf.shape[0]
    C = math.gcd(H, B)
    blk, node = lax.axis_index("blk"), lax.axis_index("node")
    z = blk // inner
    p = (blk % inner) * N + node
    bf, f32 = jnp.bfloat16, jnp.float32

    load_weight = pltpu.make_async_copy(weight_ref, weight, w_sem)
    load_weight.start()
    barrier = pltpu.get_barrier_semaphore()
    here = blk * N + node

    def greet(d, _):
        other = lax.rem(here + d, B)
        pl.semaphore_signal(
            barrier, inc=1, device_id={"blk": other // N, "node": lax.rem(other, N)},
            device_id_type=pl.DeviceIdType.MESH,
        )
        return 0

    lax.fori_loop(1, B, greet, 0)

    def peer(zz, pp):
        return {"blk": zz * inner + pp // N, "node": pp % N}

    def remote(src, dst, send, recv, zz, pp):
        return pltpu.make_async_remote_copy(
            src_ref=src, dst_ref=dst, send_sem=send, recv_sem=recv,
            device_id=peer(zz, pp), device_id_type=pl.DeviceIdType.MESH,
        )

    half = lax.broadcasted_iota(jnp.int32, (R2, WIDE), 1) < HD
    wide_half = lax.broadcasted_iota(jnp.int32, (R, WIDE), 1) < HD

    for pair in range(H // 2):
        columns = slice(pair * WIDE, (pair + 1) * WIDE)
        block = query_ref[:, columns].astype(f32)
        turned = pltpu.roll(block, HD, 1)
        qp[2 * pair] = jnp.where(half, block[:R2], turned[R2:]).astype(bf)
        qp[2 * pair + 1] = jnp.where(half, turned[:R2], block[R2:]).astype(bf)
    for pair in range(H // 2):
        columns = slice(pair * WIDE, (pair + 1) * WIDE)
        keys = key_ref[:, columns].astype(f32)
        values = value_ref[:, columns].astype(f32)
        kvp[2 * pair] = jnp.where(wide_half, keys, pltpu.roll(values, HD, 1)).astype(bf)
        kvp[2 * pair + 1] = jnp.where(wide_half, pltpu.roll(keys, HD, 1), values).astype(bf)

    pl.semaphore_wait(barrier, B - 1)

    def send_q(i, act):
        row = lax.rem((z + 1) * hg + i, H)
        zz = row // hg
        n = (row - zz * hg) * B + here
        pp = n // H
        u = n - pp * H
        mine = jnp.logical_and(zz == z, pp == p)

        @pl.when(jnp.logical_not(mine))
        def _():
            act(remote(qp.at[row], qbuf.at[u], q_send.at[row], q_recv.at[u], zz, pp))

        return mine, row, u

    def start_q(i, _):
        mine, row, u = send_q(i, lambda c: c.start())

        @pl.when(mine)
        def _():
            pltpu.make_async_copy(qp.at[row], qbuf.at[u], q_recv.at[u]).start()

        return 0

    lax.fori_loop(0, H, start_q, 0)

    def phase1(dz):
        g = lax.rem(z + dz, G)
        return remote(
            kvp.at[pl.ds(g * hg, hg)], kvz.at[dz - 1], z_send.at[dz - 1], z_recv.at[dz - 1], g, p
        )

    for dz in range(1, G):
        phase1(dz).start()

    def first(pp):
        return (pp * H) // B

    def last(pp):
        return (pp * H + H - 1) // B

    def kv_src(s, h):
        return kvp.at[z * hg + h] if s == 0 else kvz.at[s - 1, h]

    def share_kv(s, act):
        b = s * PL + p

        def one(dp, _):
            pp = lax.rem(p + dp, PL)
            for slot in range(NS):
                @pl.when(first(pp) + slot <= last(pp))
                def _():
                    act(remote(
                        kv_src(s, first(pp) + slot), kvbuf.at[slot, b],
                        kv_send.at[s, dp, slot], kv_recv.at[slot, b], z, pp,
                    ))
            return 0

        lax.fori_loop(1, PL, one, 0)

    def own_kv(s):
        b = s * PL + p
        for slot in range(NS):
            @pl.when(first(p) + slot <= last(p))
            def _():
                pltpu.make_async_copy(kv_src(s, first(p) + slot), kvbuf.at[slot, b], kv_recv.at[slot, b]).start()

    start = lambda c: c.start()
    share_kv(0, start)
    own_kv(0)

    scale = 1.0 / math.sqrt(HD)

    def take_q(u, _):
        pltpu.make_async_copy(qbuf.at[u], qbuf.at[u], q_recv.at[u]).wait()
        both = qbuf[u].astype(f32) * scale
        zero = jnp.zeros_like(both)
        qfull[u] = jnp.concatenate(
            [jnp.where(half, both, zero), jnp.where(half, pltpu.roll(both, HD, 1), zero)], axis=0
        ).astype(bf)
        return 0

    def take_kv(low, high):
        for slot in range(NS):
            @pl.when(first(p) + slot <= last(p))
            def _():
                def one(b, _):
                    pltpu.make_async_copy(kvbuf.at[slot, b], kvbuf.at[slot, b], kv_recv.at[slot, b]).wait()
                    vbuf[slot, b] = jnp.where(wide_half, jnp.ones((), bf), kvbuf[slot, b])
                    return 0
                lax.fori_loop(low * PL, high * PL, one, 0)

    def give(u, act):
        n = p * H + u
        h = n // B
        b = n - h * B
        zz, pp = b // PL, lax.rem(b, PL)
        mine = jnp.logical_and(zz == z, pp == p)
        row = z * hg + h

        @pl.when(jnp.logical_not(mine))
        def _():
            act(remote(opack.at[u], oin.at[row], o_send.at[u], o_recv.at[row], zz, pp))

        return mine, row

    def attend(low, high, t):
        slot = (p * H + t * C) // B - first(p)
        keys = kvbuf[slot, low * PL:high * PL].reshape((high - low) * PL * R, WIDE)
        values = vbuf[slot, low * PL:high * PL].reshape((high - low) * PL * R, WIDE)

        def product(c):
            return lax.dot_general(
                qfull[t * C + c], keys, (((1,), (1,)), ((), ())), preferred_element_type=f32
            )

        def soften(c, scores):
            u = t * C + c
            peak = jnp.max(scores, axis=1, keepdims=True)
            if low > 0:
                before = peaks[u]
                peak = jnp.maximum(before[:, :1], peak)
            expo = jnp.exp(scores - peak).astype(bf)
            total = jnp.dot(expo, values, preferred_element_type=f32)
            if low > 0:
                total = total + accum[u] * jnp.exp(before - peak)
            if high < G:
                peaks[u] = jnp.broadcast_to(peak, (R, WIDE))
                accum[u] = total
                return
            turned = pltpu.roll(total, HD, 1)
            opack[u] = jnp.where(
                half, turned[:R2] / total[:R2], total[R2:] / turned[R2:]
            ).astype(bf)

        scores = product(0)
        for c in range(C):
            ahead = product(c + 1) if c + 1 < C else None
            soften(c, scores)
            scores = ahead
        if high < G:
            return
        for i in range(C):
            u = t * C + i
            mine, row = give(u, start)

            @pl.when(mine)
            def _():
                pltpu.make_async_copy(opack.at[u], oin.at[row], o_recv.at[row]).start()

    def relay(s):
        if s < G:
            phase1(s).wait_recv()
            share_kv(s, start)
            own_kv(s)

    stages = [(0, 1)] + [(s, min(s + 2, G)) for s in range(1, G, 2)]
    turns = H // C
    relay(1)
    relayed = 2
    lax.fori_loop(0, H, take_q, 0)
    for low, high in stages:
        while relayed < high:
            relay(relayed)
            relayed += 1
        take_kv(low, high)

        def turn(t, _):
            attend(low, high, t)
            return 0

        if low > 0 and high < G:
            lax.fori_loop(0, turns // 2, turn, 0)
            relay(relayed)
            relayed += 1
            lax.fori_loop(turns // 2, turns, turn, 0)
        else:
            lax.fori_loop(0, turns, turn, 0)

    for dz in range(1, G):
        phase1(dz).wait_send()
    for s in range(G):
        share_kv(s, lambda c: c.wait_send())

    def end_q(i, _):
        send_q(i, lambda c: c.wait_send())
        return 0

    lax.fori_loop(0, H, end_q, 0)

    def end(u, _):
        give(u, lambda c: c.wait_send())
        pltpu.make_async_copy(oin.at[u], oin.at[u], o_recv.at[u]).wait()
        return 0

    load_weight.wait()
    lax.fori_loop(0, H, end, 0)
    for pair in range(H // 2):
        even, odd = oin[2 * pair].astype(f32), oin[2 * pair + 1].astype(f32)
        attn[:, pair * WIDE:(pair + 1) * WIDE] = jnp.concatenate(
            [
                jnp.where(half, even, pltpu.roll(odd, HD, 1)),
                jnp.where(half, pltpu.roll(even, HD, 1), odd),
            ],
            axis=0,
        ).astype(bf)
    mixed_ref[...] = jnp.dot(attn[...], weight[...], preferred_element_type=f32).astype(bf)


def per_device(query, key, value, out_weight):
    R, features = query.shape
    H = features // HD
    R2 = R // 2
    nblk, N = lax.axis_size("blk"), lax.axis_size("node")
    B = nblk * N
    G = groups_of(nblk, H)
    hg = H // G
    NS = (H + B - 2) // B + 1
    dma = pltpu.SemaphoreType.DMA
    bf, f32 = jnp.bfloat16, jnp.float32
    vmem = pl.BlockSpec(memory_space=pltpu.VMEM)
    mixed = pl.pallas_call(
        functools.partial(kernel, G, B, N),
        out_shape=jax.ShapeDtypeStruct((R, out_weight.shape[1]), bf),
        in_specs=[vmem, vmem, vmem, pl.BlockSpec(memory_space=pl.ANY)],
        out_specs=vmem,
        scratch_shapes=[
            pltpu.VMEM((H, R2, WIDE), bf),
            pltpu.VMEM((H, R, WIDE), bf),
            pltpu.VMEM((max(G - 1, 1), hg, R, WIDE), bf),
            pltpu.VMEM((H, R2, WIDE), bf),
            pltpu.VMEM((NS, B, R, WIDE), bf),
            pltpu.VMEM((NS, B, R, WIDE), bf),
            pltpu.VMEM((H, R, WIDE), bf),
            pltpu.VMEM((H, R, WIDE), f32),
            pltpu.VMEM((H, R, WIDE), f32),
            pltpu.VMEM((H, R2, WIDE), bf),
            pltpu.VMEM((H, R2, WIDE), bf),
            pltpu.VMEM((R, features), bf),
            pltpu.VMEM(out_weight.shape, bf),
            dma((max(G - 1, 1),)),
            dma((max(G - 1, 1),)),
            dma((H,)),
            dma((H,)),
            dma((G, B // G, NS)),
            dma((NS, B)),
            dma((H,)),
            dma((H,)),
            dma(()),
        ],
        compiler_params=pltpu.CompilerParams(
            collective_id=0, has_side_effects=True, vmem_limit_bytes=60 * 1024 * 1024
        ),
        name="attention",
    )(query, key, value, out_weight)
    return lax.psum_scatter(mixed, "pair", scatter_dimension=0, tiled=True)


def solution(mesh):
    in_specs = (
        P(("grp", "blk", "node"), "pair"),
        P(("grp", "blk", "node"), "pair"),
        P(("grp", "blk", "node"), "pair"),
        P("pair", None),
    )
    out_specs = P(("grp", "blk", "node", "pair"), None)
    return jax.shard_map(
        per_device, mesh=mesh, in_specs=in_specs, out_specs=out_specs, check_vma=False
    )
```
